32 devices in a mesh: wide: 8 (over y, x, core), narrow: 4 (over z).
Axes of the slice: x: 2, y: 2, z: 4, core: 2. Of those that a mesh axis runs over, the one named last changes fastest.
Arguments:
- panels: float32 [64, 512, 512], P('wide', 'narrow'), may hold values from -0.6 to 0.6
- factors: float32 [16, 512, 512], P('wide', 'narrow'), may hold values from -2 to 2
- member: int32 [16, 4], replicated, may hold values from 0 to 63, as said below
- target: int32 [16, 10], replicated, may hold values from 0 to 7
- ancestors: float32 [8, 512, 512], P('wide', 'narrow'), may hold values from -6 to 6
Outputs:
- updated: float32 [8, 512, 512], P('wide', 'narrow')
The draws below stay inside these ranges and needn't reach their ends.
Inputs may be any that keep to these rules, and one draw needn't show every extreme that they name: `member`: the blocks of supernode s are 4 distinct indices in [(s // 2) * 8, (s // 2 + 1) * 8); every block belongs to exactly one supernode.
All inputs are finite; a program needn't handle non-finite values.
Results may differ from the reference program's by a relative error of at most 0.0003.
Values sent between devices are 32-bit elements; how exact they have to be, the bound alone decides.
A program may use at most 128 MiB of HBM per device.

```python
import math
import jax
import jax.numpy as jnp
import numpy as np
from jax import lax

W = 512
NB = 4
SUP_DEV = 2
NP = 10
SUPER = 16
BLOCKS = 64
ANC = 8


def draw_factors(key, part):
    diag_key = jax.random.fold_in(key, 11)
    off_key = jax.random.fold_in(key, 12)
    diagonal = jax.random.uniform(diag_key, (SUPER, W), jnp.float32, 0.5, 2.0)
    offdiag = jnp.clip(jax.random.normal(off_key, (SUPER, W, W), jnp.float32), -6.0, 6.0) * (0.5 / jnp.sqrt(jnp.float32(W)))
    eye = jnp.eye(W, dtype=jnp.float32)
    return offdiag * (1.0 - eye)[None] + diagonal[:, :, None] * eye[None]


def draw_member(key, part):
    owners = SUPER // SUP_DEV
    keys = jax.random.split(jax.random.fold_in(key, 21), owners)
    shuffled = jax.vmap(lambda single: jax.random.permutation(single, SUP_DEV * NB))(keys)
    offsets = jnp.arange(owners, dtype=jnp.int32)[:, None] * (SUP_DEV * NB)
    return (shuffled.astype(jnp.int32) + offsets).reshape(SUPER, NB)


def with_ends(drawn, key, smallest, high):
    spot = [jax.random.randint(jax.random.fold_in(key, axis), (), 0, length) for axis, length in enumerate(drawn.shape)]
    longest = drawn.shape.index(max(drawn.shape))
    next_to = spot[:longest] + [(spot[longest] + 1) % drawn.shape[longest]] + spot[longest + 1:]
    return drawn.at[tuple(spot)].set(smallest).at[tuple(next_to)].set(high)


def steps_of(key, extent, cuts, low, top_value):
    level, own = 1.0, jax.random.fold_in(key, 6)
    for dim, parts in cuts:
        draws = jnp.exp(jax.random.uniform(jax.random.fold_in(own, dim), (parts,), jnp.float32, low / len(cuts), top_value / len(cuts)))
        level = level * jnp.repeat(draws, extent[dim] // parts).reshape([-1 if axis == dim else 1 for axis in range(len(extent))])
    return level


def rank_table(number_of, slope):
    loads = [(1 << 20) // math.isqrt(rank ** slope) + 1 for rank in range(1, number_of + 1)]
    spread = 1 + sum(loads) // (1 << 30)
    return np.cumsum(np.array([max(1, weight // spread) for weight in loads]))


def ranked_ids(stream_key, extent, number_of, skew):
    grid = rank_table(number_of, skew)
    lot = jax.random.randint(jax.random.fold_in(stream_key, 1), extent, 0, int(grid[number_of - 1]))
    standing = jnp.searchsorted(jnp.asarray(grid, jnp.int32), lot, side="right")
    return jax.random.permutation(jax.random.fold_in(stream_key, 2), number_of)[standing].astype(jnp.int32)


def gaussian(key, shape, width, most, cuts=(), kind=jnp.bfloat16):
    level = steps_of(key, shape, cuts, -0.22, 0.18) if cuts else 1.0
    values = jax.random.normal(key, shape, jnp.float32) * width * level
    return jnp.minimum(jnp.maximum(values, -most), most).astype(kind)


def setup_inputs(seed: int = 0) -> dict:
    splits = jax.random.split(jax.random.key(seed), 6)
    panels = gaussian(splits[0], (BLOCKS, W, W), 0.1, 0.6, ((0, 8), (1, 4)), jnp.float32)
    factors = draw_factors(jax.random.fold_in(splits[5], 71), 0)
    member = draw_member(jax.random.fold_in(splits[5], 71), 0)
    target = with_ends(ranked_ids(splits[3], (SUPER, NP), ANC, 2), jax.random.fold_in(splits[3], 3), 0, ANC - 1).astype(jnp.int32)
    ancestors = gaussian(splits[4], (ANC, W, W), 1.0, 6.0, ((0, 8), (1, 4)), jnp.float32)
    return {"panels": panels, "factors": factors, "member": member, "target": target, "ancestors": ancestors}


def pair_lists(count):
    left_pick = []
    right_pick = []
    for upper in range(count):
        for lower in range(upper + 1):
            left_pick.append(upper)
            right_pick.append(lower)
    return np.array(left_pick, dtype=np.int32), np.array(right_pick, dtype=np.int32)


def reference(panels, factors, member, target, ancestors):
    left_pick, right_pick = pair_lists(member.shape[1])
    highest = lax.Precision.HIGHEST

    def advance(running, inputs):
        members, factor, targets = inputs
        blocks = panels[members]
        scaled = jnp.einsum("kij,jm->kim", blocks, factor, precision=highest)
        updates = jnp.einsum("pim,pjm->pij", scaled[left_pick], scaled[right_pick], precision=highest)
        onehot = (targets[:, None] == jnp.arange(ANC, dtype=jnp.int32)[None, :]).astype(jnp.float32)
        return running + jnp.einsum("pa,pij->aij", onehot, updates, precision=highest), None

    running, ignored = lax.scan(advance, jnp.zeros((ANC, W, W), jnp.float32), (member, factors, target))
    return ancestors - running
```

```python
import functools

import jax
import jax.numpy as jnp
from jax import lax
from jax.experimental import pallas as pl
from jax.experimental.pallas import tpu as pltpu
from jax.sharding import PartitionSpec as P

MESH = pl.DeviceIdType.MESH
CORES = 2
PIECE = 32
SOURCES = 3
ROWS_DOT = (((1,), (1,)), ((), ()))
COLS_DOT = (((1,), (0,)), ((), ()))


def halves(x):
    hi = x.astype(jnp.bfloat16)
    return hi, (x - hi.astype(jnp.float32)).astype(jnp.bfloat16)


def dot3(ah, al, bh, bl, dims):
    dot = functools.partial(
        lax.dot_general, dimension_numbers=dims, preferred_element_type=jnp.float32
    )
    return dot(ah, bh) + (dot(ah, bl) + dot(al, bh))


def kernel(cfg, member, target, panels, factors, ancestors, out, pan, stage, p_recv, f_full, fh, fl,
           s_full, s_hi, s_lo, upd, portion, xy_recv, zsum, pair, z_recv, t_recv, turned,
           loc_sem, pan_sem, fs_sem, fr_sem, f2s_sem, f2r_sem, ps_sem, pr_sem, ss_sem, sr_sem,
           xs_sem, xr_sem, zs_sem, zr_sem, qs_sem, qr_sem, turn_sem):
    n, q_count, sups, nb, width, part, unit, split, pieces = cfg
    hr = part // pieces
    units = CORES * sups
    mid = units // 2
    last = units - 1
    cols = width // units
    rows_z = split * part
    wide = lax.axis_index("wide")
    z = lax.axis_index("narrow")
    core = lax.rem(wide, CORES)
    q = lax.div(wide, CORES)
    mine = lax.rem(z, unit) * CORES + core
    my_unit = lax.div(z, unit)
    half = lax.div(my_unit, mid)
    far_sender = core != half
    outer_unit = half * last
    far_outer = (1 - half) * last
    inner = my_unit != outer_unit
    supernode = q * units + my_unit

    def at(q_, core_, z_):
        return {"wide": q_ * CORES + core_, "narrow": z_}

    def order(i):
        h, j = i // mid, i % mid
        near = half * mid + lax.rem(my_unit - half * mid + j, mid)
        far = mid + j - half * (1 + 2 * j)
        return (1 - h) * near + h * far

    def remote(src, dst, send, recv, dev):
        return pltpu.make_async_remote_copy(src_ref=src, dst_ref=dst, send_sem=send, recv_sem=recv,
                                            device_id=dev, device_id_type=MESH)

    def arrived(ref, sem):
        pltpu.make_async_copy(ref, ref, sem).wait()

    def piece(h):
        return pl.ds(h * hr if isinstance(h, int) else pl.multiple_of(h * hr, hr), hr)

    pan_copy = pltpu.make_async_copy(panels, pan, pan_sem)
    pan_copy.start()
    anc_copy = pltpu.make_async_copy(ancestors.at[0], out.at[0], loc_sem)
    anc_copy.start()

    barrier = pltpu.get_barrier_semaphore()
    for i in range(1, CORES * n):
        other = lax.rem(z * CORES + core + i, CORES * n)
        pl.semaphore_signal(barrier, inc=1, device_id=at(q, lax.rem(other, CORES), lax.div(other, CORES)),
                            device_id_type=MESH)
    for i in range(1, q_count):
        pl.semaphore_signal(barrier, inc=1, device_id=at(lax.rem(q + i, q_count), core, z), device_id_type=MESH)
    pl.semaphore_wait(barrier, CORES * n - 1 + q_count - 1)

    def chip_of(s, e):
        return (core * sups + s) * unit + e // CORES

    def to_self(s, e):
        return jnp.logical_and(chip_of(s, e) == z, core == e % CORES)

    def f_source(s, e, local):
        src, dst = factors.at[s, pl.ds(e * part, part)], f_full.at[z, e]
        if local:
            return pltpu.make_async_copy(src, dst, fr_sem.at[z])
        return remote(src, dst, fs_sem.at[s, e], fr_sem.at[z], at(q, e % CORES, chip_of(s, e)))

    def nearest(i):
        return lax.rem(i + 1 - core, sups)

    def p_source(s, e, h):
        src = stage.at[s, :, pl.ds(e * part + h * hr, hr)]
        return remote(src, p_recv.at[z, h], ps_sem.at[s, e, h], pr_sem.at[z, h], at(q, e % CORES, chip_of(s, e)))

    parts = [(i, e) for i in range(sups) for e in range(split)]
    for i, e in parts:
        s = nearest(i)

        @pl.when(to_self(s, e))
        def _():
            f_source(s, e, True).start()

        @pl.when(jnp.logical_not(to_self(s, e)))
        def _():
            f_source(s, e, False).start()

    pan_copy.wait()

    def pick(i, carry):
        s, k = lax.div(i, nb), lax.rem(i, nb)
        stage[s, k] = pan[lax.rem(member[wide * sups + s, k], sups * nb)]
        return carry

    lax.fori_loop(0, sups * nb, pick, 0)

    far_inner = jnp.logical_and(far_sender, inner)
    far_outer_sender = jnp.logical_and(far_sender, jnp.logical_not(inner))
    p_list = [(i, e, h) for h in range(pieces) for i, e in parts]

    def send_panels():
        for i, e, h in p_list:
            s = nearest(i)

            @pl.when(to_self(s, e))
            def _():
                p_recv[z, h] = stage[s, :, pl.ds(e * part + h * hr, hr)]

            @pl.when(jnp.logical_not(to_self(s, e)))
            def _():
                p_source(s, e, h).start()

    pl.when(jnp.logical_not(far_outer_sender))(send_panels)

    for i in range(n):
        arrived(f_full.at[i, mine], fr_sem.at[i])

    def peer(i):
        other = lax.rem(mine + i, split)
        return other, at(q, lax.rem(other, CORES), my_unit * unit + lax.div(other, CORES))

    f_copies = []
    for i in range(1, split):
        other, dev = peer(i)
        f_copies.append(remote(f_full.at[:, mine], f_full.at[:, mine], f2s_sem.at[other], f2r_sem.at[mine], dev))
        f_copies[-1].start()
    for i in range(1, split):
        other, dev = peer(i)
        arrived(f_full.at[:, other], f2r_sem.at[other])
    hi, lo = halves(f_full[...].reshape(width, width))
    fh[...] = hi
    fl[...] = lo

    def s_copy(zz, h, j):
        other, dev = peer(j)
        ref = s_full.at[:, zz, mine, piece(h)]
        return remote(ref, ref, ss_sem.at[zz, h, other], sr_sem.at[zz, h, mine], dev)

    def scale(zz, h):
        @pl.when(jnp.logical_not(jnp.logical_and(zz == z, core == half)))
        def _():
            arrived(p_recv.at[zz, h], pr_sem.at[zz, h])

        ph, plo = halves(p_recv[zz, h].reshape(nb * hr, width))
        s = dot3(ph, plo, fh[...], fl[...], COLS_DOT).reshape(nb, hr, width)
        s_full[:, zz, mine, piece(h)] = s
        for j in range(1, split):
            s_copy(zz, h, j).start()
        s_hi[:, zz, mine, piece(h)], s_lo[:, zz, mine, piece(h)] = halves(s)

    def take(zz, h):
        for j in range(1, split):
            other, dev = peer(j)
            arrived(s_full.at[:, zz, other, piece(h)], sr_sem.at[zz, h, other])
            s_hi[:, zz, other, piece(h)], s_lo[:, zz, other, piece(h)] = halves(s_full[:, zz, other, piece(h)])

    def scale_all(a):
        def one(i, carry):
            scale(a * unit + lax.div(i, pieces), lax.rem(i, pieces))
            return carry

        def two(i, carry):
            take(a * unit + lax.div(i, pieces), lax.rem(i, pieces))
            return carry

        lax.fori_loop(0, unit * pieces, one, 0)
        lax.fori_loop(0, unit * pieces, two, 0)

    def xy_copy(r, c, h, other):
        return remote(portion.at[r, c, h, pl.ds(other * CORES, CORES)], xy_recv.at[q, r, c, h],
                      xs_sem.at[other, r, c, h], xr_sem.at[q, r, c, h], at(other, core, z))

    two = nb // 2

    def block(a, b, h=None, flip=False):
        rows = unit * (part if h is None else hr)
        bz, az = pl.ds(b * unit, unit), pl.ds(a * unit, unit)
        for first in range(0, nb, two):
            lo_k, hi_k = (0, first + two) if flip else (first, nb)
            ks, ls = pl.ds(lo_k, hi_k - lo_k), pl.ds(first, two)
            left = [(r[ks, az, mine] if h is None else r[ks, az, mine, piece(h)]).reshape((hi_k - lo_k) * rows, width)
                    for r in (s_hi, s_lo)]
            right = [r[ls, bz].reshape(two * cols, width) for r in (s_hi, s_lo)]
            upd[lo_k * rows:hi_k * rows, first * cols:(first + two) * cols] = dot3(*left, *right, ROWS_DOT)
        r, c = (b, a) if flip else (a, b)

        def tiles(i, carry):
            other = lax.rem(q + 1 + i, q_count)
            sums = [None] * CORES
            p = 0
            for k in range(nb):
                for l in range(k + 1):
                    x, y = (l, k) if flip else (k, l)
                    u = upd[x * rows:(x + 1) * rows, y * cols:(y + 1) * cols]
                    for t in range(CORES):
                        term = (target[supernode, p] == other * CORES + t).astype(jnp.float32) * u
                        sums[t] = term if p == 0 else sums[t] + term
                    p += 1
            hs = range(pieces) if h is None else (h,)
            for t in range(CORES):
                for m in range(unit):
                    for g, hh in enumerate(hs):
                        first = (m * len(hs) + g) * hr
                        portion[r, c, hh, other * CORES + t, m] = sums[t][first:first + hr]

            @pl.when(other != q)
            def _():
                for hh in hs:
                    xy_copy(r, c, hh, other).start()

            return carry

        lax.fori_loop(0, q_count, tiles, 0)

    def item(i, j):
        new_row = j <= i
        return (order(jnp.where(new_row, i, j - i - 1)), order(jnp.where(new_row, j, i)))

    def step(i):
        scale_all(order(i))

        def one(j, carry):
            block(*item(i, j))
            return carry

        lax.fori_loop(0, 2 * i + 1, one, 0)

    def last_item(j):
        newest = j < last
        other = order(lax.rem(j, last))
        return jnp.where(newest, far_outer, other), jnp.where(newest, other, far_outer)

    def last_step(h):
        for m in range(unit):
            scale(far_outer * unit + m, h)
        for m in range(unit):
            take(far_outer * unit + m, h)

        def one(j, carry):
            block(far_outer, order(j), h)
            return carry

        def flipped(j, carry):
            block(far_outer, order(j), h, True)
            return carry

        lax.fori_loop(0, last, one, 0)
        lax.fori_loop(0, last, flipped, 0)

    def is_near(r):
        return lax.div(r, mid) == half

    def deliver(r, c, h, what):
        near = is_near(r)
        src = jnp.where(near, jnp.where(r == my_unit, 0, 1), SOURCES - 1)
        flip = jnp.logical_and(c == far_outer, r != far_outer)
        for t in range(CORES):
            for m in range(unit):
                zz = r * unit + m
                own = jnp.logical_and(zz == z, core == t)
                send, recv, dev = zs_sem.at[r, c, h, t, m], zr_sem.at[src, c, mine, h], at(q, t, zz)
                plain = remote(zsum.at[r, c, h, t, m], z_recv.at[src, c, mine, h], send, recv, dev)
                flipped = remote(zsum.at[r, c, h, t], t_recv.at[src, :, mine, h], send, recv, dev)

                if what == "start":
                    @pl.when(jnp.logical_and(own, jnp.logical_not(flip)))
                    def _():
                        z_recv[0, c, mine, h] = zsum[r, c, h, t, m]

                    @pl.when(jnp.logical_and(own, flip))
                    def _():
                        t_recv[0, :, mine, h] = zsum[r, c, h, t]

                @pl.when(jnp.logical_and(jnp.logical_not(own), jnp.logical_not(flip)))
                def _():
                    plain.start() if what == "start" else plain.wait_send()

                @pl.when(jnp.logical_and(jnp.logical_not(own), flip))
                def _():
                    flipped.start() if what == "start" else flipped.wait_send()

    def pair_copy(r, c, h):
        f = lax.rem(r, mid)
        dev = at(q, core, z + unit - 2 * unit * half)
        return remote(zsum.at[r, c, h], pair.at[f, c, h], qs_sem.at[f, c, h], qr_sem.at[f, c, h], dev)

    def gather(r, c, h):
        total = portion[r, c, h, pl.ds(q * CORES, CORES)]
        for j in range(1, q_count):
            other = lax.rem(q + j, q_count)
            arrived(xy_recv.at[other, r, c, h], xr_sem.at[other, r, c, h])
            total = total + xy_recv[other, r, c, h]
        zsum[r, c, h] = total

        @pl.when(is_near(r))
        def _():
            deliver(r, c, h, "start")

        @pl.when(jnp.logical_not(jnp.logical_or(is_near(r), inner)))
        def _():
            pair_copy(r, c, h).start()

    def join(r, c, h):
        @pl.when(jnp.logical_and(inner, jnp.logical_not(is_near(r))))
        def _():
            f = lax.rem(r, mid)
            arrived(pair.at[f, c, h], qr_sem.at[f, c, h])
            zsum[r, c, h] = zsum[r, c, h] + pair[f, c, h]
            deliver(r, c, h, "start")

    def over(do, i):
        def one(j, carry):
            do(*item(i, lax.div(j, pieces)), lax.rem(j, pieces))
            return carry

        lax.fori_loop(0, (2 * i + 1) * pieces, one, 0)

    def over_last(do, h):
        def one(j, carry):
            do(*last_item(j), h)
            return carry

        lax.fori_loop(0, 2 * last, one, 0)

    def over_corner(do):
        def one(h, carry):
            do(far_outer, far_outer, h)
            return carry

        lax.fori_loop(0, pieces, one, 0)

    step(0)
    step(1)

    @pl.when(far_inner)
    def _():
        for i, e, h in p_list[:-1]:
            p_source(nearest(i), e, h).wait_send()
        pl.semaphore_signal(turn_sem, inc=1, device_id=at(q, core, z - unit + 2 * unit * half),
                            device_id_type=MESH)

    @pl.when(far_outer_sender)
    def _():
        pl.semaphore_wait(turn_sem, 1)
        send_panels()

    step(2)
    over(gather, 0)
    over(gather, 1)
    for h in range(pieces):
        last_step(h)
        if h == 0:
            over(gather, 2)
    block(far_outer, far_outer)
    over(join, 2)
    for h in range(pieces):
        over_last(gather, h)
        over_last(join, h)
    over_corner(gather)
    over_corner(join)

    anc_copy.wait()
    row0 = pl.multiple_of(lax.rem(z, unit) * rows_z, rows_z)
    for src in range(SOURCES):
        outermost = far_outer if src < SOURCES - 1 else outer_unit
        for c in range(units):
            flip = outermost == c
            if src == SOURCES - 1:
                flip = jnp.logical_and(flip, inner)

            def wait(flipped):
                for e in range(split):
                    for h in range(pieces):
                        def one():
                            arrived(t_recv.at[src, :, e, h] if flipped else z_recv.at[src, c, e, h],
                                    zr_sem.at[src, c, e, h])

                        one() if src else pl.when(mine != e)(one)

            @pl.when(flip)
            def _():
                wait(True)
                turned[...] = t_recv[src].reshape(cols, cols).T
                out[0, :, c * cols:(c + 1) * cols] = (
                    out[0, :, c * cols:(c + 1) * cols] - turned[pl.ds(row0, rows_z)])

            @pl.when(jnp.logical_not(flip))
            def _():
                wait(False)
                out[0, :, c * cols:(c + 1) * cols] = (
                    out[0, :, c * cols:(c + 1) * cols] - z_recv[src, c].reshape(rows_z, cols))

    for i, e in parts:
        s = nearest(i)

        @pl.when(jnp.logical_not(to_self(s, e)))
        def _():
            f_source(s, e, False).wait_send()

    for i, e, h in p_list[:-1]:
        s = nearest(i)

        @pl.when(jnp.logical_not(jnp.logical_or(to_self(s, e), far_inner)))
        def _():
            p_source(s, e, h).wait_send()

    i, e, h = p_list[-1]

    @pl.when(jnp.logical_not(to_self(nearest(i), e)))
    def _():
        p_source(nearest(i), e, h).wait_send()

    for copy in f_copies:
        copy.wait_send()

    def sent(i, carry):
        for j in range(1, split):
            s_copy(lax.div(i, pieces), lax.rem(i, pieces), j).wait_send()
        return carry

    lax.fori_loop(0, n * pieces, sent, 0)

    def sent_sums(i, carry):
        h, c, r = lax.rem(i, pieces), lax.rem(lax.div(i, pieces), units), lax.div(i, pieces * units)
        for j in range(1, q_count):
            xy_copy(r, c, h, lax.rem(q + j, q_count)).wait_send()

        @pl.when(jnp.logical_or(is_near(r), inner))
        def _():
            deliver(r, c, h, "wait")

        @pl.when(jnp.logical_not(jnp.logical_or(is_near(r), inner)))
        def _():
            pair_copy(r, c, h).wait_send()

        return carry

    lax.fori_loop(0, units * units * pieces, sent_sums, 0)


def shards(panels, factors, member, target, ancestors):
    sups, blk_count, nb = factors.shape[0], panels.shape[0], member.shape[1]
    width = panels.shape[2]
    n, wide_count = lax.axis_size("narrow"), lax.axis_size("wide")
    q_count = wide_count // CORES
    tile_count = ancestors.shape[0] * wide_count
    assert ancestors.shape[0] == 1 and n % (CORES * sups) == 0 and nb % 2 == 0 and sups == 2
    assert blk_count == sups * nb
    unit = n // (CORES * sups)
    split = unit * CORES
    part = panels.shape[1] // split
    pieces = max(1, part // PIECE)
    hr = part // pieces
    units = CORES * sups
    cols = width // units
    f32, bf16 = jnp.float32, jnp.bfloat16
    dma = pltpu.SemaphoreType.DMA
    cfg = (n, q_count, sups, nb, width, part, unit, split, pieces)
    any_space = pl.BlockSpec(memory_space=pl.ANY)
    smem = pl.BlockSpec(memory_space=pltpu.SMEM)
    return pl.pallas_call(
        functools.partial(kernel, cfg),
        out_shape=jax.ShapeDtypeStruct(ancestors.shape, f32),
        in_specs=[smem, smem, any_space, any_space, any_space],
        out_specs=pl.BlockSpec(memory_space=pltpu.VMEM),
        scratch_shapes=[
            pltpu.VMEM(panels.shape, f32),
            pltpu.VMEM((sups, nb, panels.shape[1], width), f32),
            pltpu.VMEM((n, pieces, nb, hr, width), f32),
            pltpu.VMEM((n, split, part, width), f32),
            pltpu.VMEM((width, width), bf16),
            pltpu.VMEM((width, width), bf16),
            pltpu.VMEM((nb, n, split, part, width), f32),
            pltpu.VMEM((nb, n, split, part, width), bf16),
            pltpu.VMEM((nb, n, split, part, width), bf16),
            pltpu.VMEM((nb * unit * part, nb * cols), f32),
            pltpu.VMEM((units, units, pieces, tile_count, unit, hr, cols), f32),
            pltpu.VMEM((q_count, units, units, pieces, CORES, unit, hr, cols), f32),
            pltpu.VMEM((units, units, pieces, CORES, unit, hr, cols), f32),
            pltpu.VMEM((units // 2, units, pieces, CORES, unit, hr, cols), f32),
            pltpu.VMEM((SOURCES, units, split, pieces, hr, cols), f32),
            pltpu.VMEM((SOURCES, unit, split, pieces, hr, cols), f32),
            pltpu.VMEM((cols, cols), f32),
            dma, dma,
            dma((sups, split)), dma((n,)),
            dma((split,)), dma((split,)),
            dma((sups, split, pieces)), dma((n, pieces)),
            dma((n, pieces, split)), dma((n, pieces, split)),
            dma((q_count, units, units, pieces)), dma((q_count, units, units, pieces)),
            dma((units, units, pieces, CORES, unit)), dma((SOURCES, units, split, pieces)),
            dma((units // 2, units, pieces)), dma((units // 2, units, pieces)),
            pltpu.SemaphoreType.REGULAR,
        ],
        compiler_params=pltpu.CompilerParams(
            collective_id=0, has_side_effects=True, vmem_limit_bytes=58 * 2**20
        ),
        name="level",
    )(member, target, panels, factors, ancestors)


def solution(mesh):
    return jax.shard_map(
        shards,
        mesh=mesh,
        in_specs=(
            P("wide", "narrow", None),
            P("wide", "narrow", None),
            P(),
            P(),
            P("wide", "narrow", None),
        ),
        out_specs=P("wide", "narrow", None),
        check_vma=False,
    )
```

```python
import functools
import math

import jax
import jax.numpy as jnp
from jax import lax
from jax.experimental import pallas as pl
from jax.experimental.pallas import tpu as pltpu
from jax.sharding import PartitionSpec as P

MESH = pl.DeviceIdType.MESH
CORES = 2
PIECE = 32
SOURCES = 3
ROWS_DOT = (((1,), (1,)), ((), ()))
COLS_DOT = (((1,), (0,)), ((), ()))


def halves(x):
    hi = x.astype(jnp.bfloat16)
    return hi, (x - hi.astype(jnp.float32)).astype(jnp.bfloat16)


def dot3(ah, al, bh, bl, dims):
    dot = functools.partial(
        lax.dot_general, dimension_numbers=dims, preferred_element_type=jnp.float32
    )
    return dot(ah, bh) + (dot(ah, bl) + dot(al, bh))


def kernel(cfg, member, target, panels, factors, ancestors, out, pan, stage, p_recv, f_full, fh, fl,
           s_full, s_hi, s_lo, upd, portion, recv1, recv2, zsum, pair, z_recv, t_recv, turned, relay,
           loc_sem, pan_sem, fs_sem, fr_sem, f2s_sem, f2r_sem, ps_sem, pr_sem, ss_sem, sr_sem,
           xs1_sem, xr1_sem, xs2_sem, xr2_sem, zs_sem, zr_sem, qs_sem, qr_sem, rr_sem, rf_sem):
    n, side, sups, nb, width, part, unit, split, pieces = cfg
    hr = part // pieces
    units = CORES * sups
    mid = units // 2
    last = units - 1
    cols = width // units
    rows_z = split * part
    wide = lax.axis_index("wide")
    z = lax.axis_index("narrow")
    core = lax.rem(wide, CORES)
    q = lax.div(wide, CORES)
    mine = lax.rem(z, unit) * CORES + core
    my_unit = lax.div(z, unit)
    half = lax.div(my_unit, mid)
    far_sender = core != half
    outer_unit = half * last
    far_outer = (1 - half) * last
    inner = my_unit != outer_unit
    supernode = q * units + my_unit
    row, col = lax.div(q, side), lax.rem(q, side)

    def at(q_, core_, z_):
        return {"wide": q_ * CORES + core_, "narrow": z_}

    def order(i):
        h, j = i // mid, i % mid
        near = half * mid + lax.rem(my_unit - half * mid + j, mid)
        far = mid + j - half * (1 + 2 * j)
        return (1 - h) * near + h * far

    def remote(src, dst, send, recv, dev):
        return pltpu.make_async_remote_copy(src_ref=src, dst_ref=dst, send_sem=send, recv_sem=recv,
                                            device_id=dev, device_id_type=MESH)

    def arrived(ref, sem):
        pltpu.make_async_copy(ref, ref, sem).wait()

    def piece(h):
        return pl.ds(h * hr if isinstance(h, int) else pl.multiple_of(h * hr, hr), hr)

    pan_copy = pltpu.make_async_copy(panels, pan, pan_sem)
    pan_copy.start()
    anc_copy = pltpu.make_async_copy(ancestors.at[0], out.at[0], loc_sem)
    anc_copy.start()

    barrier = pltpu.get_barrier_semaphore()
    for i in range(1, CORES * n):
        other = lax.rem(z * CORES + core + i, CORES * n)
        pl.semaphore_signal(barrier, inc=1, device_id=at(q, lax.rem(other, CORES), lax.div(other, CORES)),
                            device_id_type=MESH)
    for i in range(1, side):
        for other in (row * side + lax.rem(col + i, side), lax.rem(row + i, side) * side + col):
            pl.semaphore_signal(barrier, inc=1, device_id=at(other, core, z), device_id_type=MESH)
    pl.semaphore_wait(barrier, CORES * n - 1 + 2 * (side - 1))

    def chip_of(s, e):
        return (core * sups + s) * unit + e // CORES

    def to_self(s, e):
        return jnp.logical_and(chip_of(s, e) == z, core == e % CORES)

    def f_source(s, e, local):
        src, dst = factors.at[s, pl.ds(e * part, part)], f_full.at[z, e]
        if local:
            return pltpu.make_async_copy(src, dst, fr_sem)
        return remote(src, dst, fs_sem, fr_sem, at(q, e % CORES, chip_of(s, e)))

    def nearest(i):
        return lax.rem(i + 1 - core, sups)

    def p_source(s, e, h):
        src = stage.at[s, :, pl.ds(e * part + h * hr, hr)]
        return remote(src, p_recv.at[z, h], ps_sem, pr_sem.at[z, h], at(q, e % CORES, chip_of(s, e)))

    parts = [(i, e) for i in range(sups) for e in range(split)]
    for i, e in parts:
        s = nearest(sups - 1 - i)

        @pl.when(to_self(s, e))
        def _():
            f_source(s, e, True).start()

        @pl.when(jnp.logical_not(to_self(s, e)))
        def _():
            f_source(s, e, False).start()

    pan_copy.wait()

    def pick(i, carry):
        s, k = lax.div(i, nb), lax.rem(i, nb)
        stage[s, k] = pan[lax.rem(member[wide * sups + s, k], sups * nb)]
        return carry

    lax.fori_loop(0, sups * nb, pick, 0)

    far_inner = jnp.logical_and(far_sender, inner)
    far_outer_sender = jnp.logical_and(far_sender, jnp.logical_not(inner))
    p_list = [(i, e, h) for i in range(sups) for h in range(pieces) for e in range(split)]
    relay_list = [(i, e, h) for h in range(pieces) for i in reversed(range(sups)) for e in range(split)]
    ahead = relay_list[:sups * split * max(1, pieces // 2)]

    def slot(s, e, h):
        return (s * split + e) * pieces + h

    def to_relay(i, e, h):
        s = nearest(i)
        src = stage.at[s, :, pl.ds(e * part + h * hr, hr)]
        return remote(src, relay.at[slot(s, e, h)], ps_sem, rr_sem.at[slot(s, e, h)],
                      at(q, core, z + unit - 2 * unit * half))

    def from_relay(i, e, h):
        s, outer_z = nearest(i), z - unit + 2 * unit * half
        return remote(relay.at[slot(s, e, h)], p_recv.at[outer_z, h], rf_sem, pr_sem.at[outer_z, h],
                      at(q, e % CORES, chip_of(s, e)))

    def send_relay():
        for which in relay_list:
            to_relay(*which).start()

    def pass_on(some):
        for i, e, h in some:
            which = slot(nearest(i), e, h)
            arrived(relay.at[which], rr_sem.at[which])
            from_relay(i, e, h).start()

    def send_panels():
        for i, e, h in p_list:
            s = nearest(i)

            @pl.when(to_self(s, e))
            def _():
                p_recv[z, h] = stage[s, :, pl.ds(e * part + h * hr, hr)]

            @pl.when(jnp.logical_not(to_self(s, e)))
            def _():
                p_source(s, e, h).start()

    pl.when(jnp.logical_not(far_outer_sender))(send_panels)

    arrived(f_full.at[:, mine], fr_sem)

    def peer(i):
        other = lax.rem(mine + i, split)
        return other, at(q, lax.rem(other, CORES), my_unit * unit + lax.div(other, CORES))

    f_copies = []
    for i in range(1, split):
        other, dev = peer(i)
        f_copies.append(remote(f_full.at[:, mine], f_full.at[:, mine], f2s_sem, f2r_sem, dev))
        f_copies[-1].start()
    others = pl.ds(0, split - 1)
    arrived(f_full.at[:, others], f2r_sem)
    hi, lo = halves(f_full[...].reshape(width, width))
    fh[...] = hi
    fl[...] = lo

    def s_copy(zz, h, j):
        other, dev = peer(j)
        ref = s_full.at[:, zz, mine, piece(h)]
        return remote(ref, ref, ss_sem, sr_sem.at[zz, h], dev)

    def scale(zz, h):
        @pl.when(jnp.logical_not(jnp.logical_and(zz == z, core == half)))
        def _():
            arrived(p_recv.at[zz, h], pr_sem.at[zz, h])

        ph, plo = halves(p_recv[zz, h].reshape(nb * hr, width))
        s = dot3(ph, plo, fh[...], fl[...], COLS_DOT).reshape(nb, hr, width)
        s_full[:, zz, mine, piece(h)] = s
        for j in range(1, split):
            s_copy(zz, h, j).start()
        s_hi[:, zz, mine, piece(h)], s_lo[:, zz, mine, piece(h)] = halves(s)

    def take(zz, h):
        arrived(s_full.at[:, zz, others, piece(h)], sr_sem.at[zz, h])
        for j in range(1, split):
            other, _ = peer(j)
            s_hi[:, zz, other, piece(h)], s_lo[:, zz, other, piece(h)] = halves(s_full[:, zz, other, piece(h)])

    def scale_all(a, between=None):
        def one(i, carry):
            scale(a * unit + lax.div(i, pieces), lax.rem(i, pieces))
            return carry

        def two(i, carry):
            take(a * unit + lax.div(i, pieces), lax.rem(i, pieces))
            return carry

        lax.fori_loop(0, unit * pieces, one, 0)
        if between is not None:
            between()
        lax.fori_loop(0, unit * pieces, two, 0)

    def place(r, c, h):
        along_row = jnp.logical_or(r > c, jnp.logical_and(r == c, h == 0))
        return along_row, jnp.where(along_row, col, row), jnp.where(along_row, row, col)

    def q_at(along_row, f, g):
        return jnp.where(along_row, g * side + f, f * side + g)

    def steps(src, dst):
        return lax.rem(src - dst - 1 + side, side)

    def mark(r, c, h):
        in_pieces = jnp.logical_and(r != c, jnp.logical_or(r == far_outer, c == far_outer))
        other = r + c - far_outer
        return (jnp.where(in_pieces, jnp.where(h == 0, far_outer, other), r),
                jnp.where(in_pieces, jnp.where(h == 0, other, far_outer), c))

    def first_copy(r, c, h, f):
        along_row, mine_f, mine_g = place(r, c, h)
        d = steps(mine_f, f)
        return remote(portion.at[r, c, h, pl.ds(f * side * CORES, side * CORES)], recv1.at[r, c, h, d],
                      xs1_sem, xr1_sem.at[*mark(r, c, h), d], at(q_at(along_row, f, mine_g), core, z))

    def second_copy(r, c, h, g):
        along_row, mine_f, mine_g = place(r, c, h)
        d = steps(mine_g, g)
        return remote(portion.at[r, c, h, pl.ds((mine_f * side + g) * CORES, CORES)], recv2.at[r, c, h, d],
                      xs2_sem, xr2_sem.at[*mark(r, c, h), d], at(q_at(along_row, mine_f, g), core, z))

    two = nb // 2

    def products(a, b, h=None):
        rows = unit * (part if h is None else hr)
        bz, az = pl.ds(b * unit, unit), pl.ds(a * unit, unit)
        for first in range(0, nb, two):
            low = first if h is None else 0
            ks, ls = pl.ds(low, nb - low), pl.ds(first, two)
            left = [(r[ks, az, mine] if h is None else r[ks, az, mine, piece(h)]).reshape((nb - low) * rows, width)
                    for r in (s_hi, s_lo)]
            right = [r[ls, bz].reshape(two * cols, width) for r in (s_hi, s_lo)]
            upd[low * rows:nb * rows, first * cols:(first + two) * cols] = dot3(*left, *right, ROWS_DOT)

    def sums_of(r, c, h=None, flip=False):
        hs = range(pieces) if h is None else (h,)
        rows = unit * len(hs) * hr

        def tiles(i, carry):
            i = lax.rem(q + 1 + i, side * side)
            oq, og = lax.div(i, side), lax.rem(i, side)
            sums = [None] * CORES
            p = 0
            for k in range(nb):
                for l in range(k + 1):
                    x, y = (l, k) if flip else (k, l)
                    u = upd[x * rows:(x + 1) * rows, y * cols:(y + 1) * cols]
                    for t in range(CORES):
                        term = (target[supernode, p] == i * CORES + t).astype(jnp.float32) * u
                        sums[t] = term if p == 0 else sums[t] + term
                    p += 1
            for x, hh in enumerate(hs):
                along_row, mine_f, mine_g = place(r, c, hh)
                f, g = jnp.where(along_row, og, oq), jnp.where(along_row, oq, og)
                for t in range(CORES):
                    for m in range(unit):
                        first = (m * len(hs) + x) * hr
                        portion[r, c, hh, (f * side + g) * CORES + t, m] = sums[t][first:first + hr]
            return carry

        lax.fori_loop(0, side * side, tiles, 0)
        for hh in hs:
            _, mine_f, _ = place(r, c, hh)
            for j in range(1, side):
                first_copy(r, c, hh, lax.rem(mine_f + j, side)).start()

    def block(a, b):
        products(a, b)
        sums_of(a, b)

    def item(i, j):
        new_row = j <= i
        return (order(jnp.where(new_row, i, j - i - 1)), order(jnp.where(new_row, j, i)))

    def step(i):
        scale_all(order(i), (lambda: pl.when(far_outer_sender)(send_relay)) if i == 1 else None)

        def one(j, carry):
            block(*item(i, j))
            return carry

        lax.fori_loop(0, 2 * i + 1, one, 0)

    def last_step(h, between=None):
        for m in range(unit):
            scale(far_outer * unit + m, h)
        if between is not None:
            between()
        for m in range(unit):
            take(far_outer * unit + m, h)

        def one(j, carry):
            products(far_outer, order(j), h)
            sums_of(far_outer, order(j), h)
            sums_of(order(j), far_outer, h, True)
            return carry

        lax.fori_loop(0, last, one, 0)

    def is_near(r):
        return lax.div(r, mid) == half

    def total_at(r, c, h, t=0, m=0):
        return (((r * units + c) * pieces + h) * CORES + t) * unit + m

    def deliver(r, c, h):
        near = is_near(r)
        src = jnp.where(near, jnp.where(r == my_unit, 0, 1), SOURCES - 1)
        flip = jnp.logical_and(c == far_outer, r != far_outer)
        for t in range(CORES):
            for m in range(unit):
                zz = r * unit + m
                own = jnp.logical_and(zz == z, core == t)
                send, recv, dev = zs_sem, zr_sem.at[src], at(q, t, zz)
                plain = remote(zsum.at[total_at(r, c, h, t, m)], z_recv.at[src, c, mine, h], send, recv, dev)
                flipped = remote(zsum.at[pl.ds(total_at(r, c, h, t), unit)], t_recv.at[src, :, mine, h], send, recv, dev)

                @pl.when(jnp.logical_and(own, jnp.logical_not(flip)))
                def _():
                    z_recv[0, c, mine, h] = zsum[total_at(r, c, h, t, m)]

                @pl.when(jnp.logical_and(own, flip))
                def _():
                    t_recv[0, :, mine, h] = zsum[pl.ds(total_at(r, c, h, t), unit)]

                @pl.when(jnp.logical_and(jnp.logical_not(own), jnp.logical_not(flip)))
                def _():
                    plain.start()

                @pl.when(jnp.logical_and(jnp.logical_not(own), flip))
                def _():
                    flipped.start()

    both = CORES * unit

    def sums_at(r, c, h):
        return pl.ds(total_at(r, c, h), both)

    def pair_copy(r, c, h, phase):
        return remote(zsum.at[sums_at(r, c, h)], pair.at[sums_at(lax.rem(r, mid), c, h)], qs_sem, qr_sem.at[phase],
                      at(q, core, z + unit - 2 * unit * half))

    def halfway(r, c, h):
        _, mine_f, mine_g = place(r, c, h)
        own = pl.ds(mine_f * side * CORES, side * CORES)
        total = portion[r, c, h, own]
        for d in range(side - 1):
            total = total + recv1[r, c, h, d]
        portion[r, c, h, own] = total
        for j in range(1, side):
            second_copy(r, c, h, lax.rem(mine_g + j, side)).start()

    def gather(r, c, h, phase):
        _, mine_f, mine_g = place(r, c, h)
        total = portion[r, c, h, pl.ds((mine_f * side + mine_g) * CORES, CORES)]
        for d in range(side - 1):
            total = total + recv2[r, c, h, d]
        zsum[sums_at(r, c, h)] = total.reshape(both, hr, cols)

        @pl.when(is_near(r))
        def _():
            deliver(r, c, h)

        @pl.when(jnp.logical_not(jnp.logical_or(is_near(r), inner)))
        def _():
            pair_copy(r, c, h, phase).start()

    def join(r, c, h):
        @pl.when(jnp.logical_not(is_near(r)))
        def _():
            zsum[sums_at(r, c, h)] = zsum[sums_at(r, c, h)] + pair[sums_at(lax.rem(r, mid), c, h)]
            deliver(r, c, h)

    def came(recv, sem, r, c, h=None):
        for d in range(side - 1):
            ref = recv.at[r, c, :, d] if h is None else recv.at[0, pl.ds(0, 2), 0, d]
            arrived(ref, sem.at[*(mark(r, c, h) if h is not None else (r, c)), d])

    def over(do, i, recv=None, sem=None):
        def one(j, carry):
            r, c = item(i, j)
            if sem is not None:
                came(recv, sem, r, c)
            for h in range(pieces):
                do(r, c, h)
            return carry

        lax.fori_loop(0, 2 * i + 1, one, 0)

    def over_last(do, h, recv=None, sem=None):
        def one(j, carry):
            a = order(j)
            if sem is not None:
                came(recv, sem, far_outer, a, h)
            do(far_outer, a, h)
            do(a, far_outer, h)
            return carry

        lax.fori_loop(0, last, one, 0)

    def over_corner(do, recv=None, sem=None):
        if sem is not None:
            came(recv, sem, far_outer, far_outer)
        for h in range(pieces):
            do(far_outer, far_outer, h)

    def in_phase(phase):
        return lambda r, c, h: gather(r, c, h, phase)

    def joined(phase, count, run):
        @pl.when(inner)
        def _():
            arrived(pair.at[pl.ds(0, count * both)], qr_sem.at[phase])
            run()

    step(0)
    step(1)
    pl.when(far_inner)(lambda: pass_on(ahead))
    over(halfway, 0, recv1, xr1_sem)
    over(halfway, 1, recv1, xr1_sem)
    step(2)
    pl.when(far_inner)(lambda: pass_on(relay_list[len(ahead):]))
    over(in_phase(0), 0, recv2, xr2_sem)
    over(in_phase(0), 1, recv2, xr2_sem)
    for h in range(pieces - 1):
        last_step(h)
        over(halfway, 2, recv1, xr1_sem)
        over_last(halfway, h, recv1, xr1_sem)
    if pieces == 1:
        over(halfway, 2, recv1, xr1_sem)
    last_step(pieces - 1, lambda: over(in_phase(0), 2, recv2, xr2_sem))
    joined(0, last * pieces, lambda: over(join, 2))
    block(far_outer, far_outer)
    for h in range(pieces - 1):
        over_last(in_phase(1 + h), h, recv2, xr2_sem)
    over_last(halfway, pieces - 1, recv1, xr1_sem)
    for h in range(pieces - 1):
        joined(1 + h, last + 1, lambda h=h: over_last(join, h))
    over_corner(halfway, recv1, xr1_sem)
    over_last(in_phase(pieces), pieces - 1, recv2, xr2_sem)
    joined(pieces, last + 1, lambda: over_last(join, pieces - 1))
    over_corner(in_phase(pieces + 1), recv2, xr2_sem)
    joined(pieces + 1, pieces, lambda: over_corner(join))

    one_each = last + unit
    pl.when(far_sender)(lambda: arrived(f_full.at[:, 0], fs_sem))
    pl.when(jnp.logical_not(far_sender))(lambda: arrived(f_full.at[pl.ds(0, n - 1), 0], fs_sem))
    pl.when(far_sender)(lambda: arrived(relay, ps_sem))
    pl.when(jnp.logical_not(far_sender))(lambda: arrived(relay.at[pl.ds(0, (n - 1) * pieces)], ps_sem))
    pl.when(far_inner)(lambda: arrived(relay, rf_sem))
    arrived(f_full.at[:, others], f2s_sem)
    arrived(s_full.at[:, :, others], ss_sem)
    arrived(recv1, xs1_sem)
    arrived(recv2, xs2_sem)
    near_count = pieces * one_each * (mid * both - 1)
    far_count = pieces * both * (one_each + (mid - 1) * units)
    pl.when(inner)(lambda: arrived(zsum.at[pl.ds(0, near_count + far_count)], zs_sem))

    @pl.when(jnp.logical_not(inner))
    def _():
        arrived(zsum.at[pl.ds(0, near_count)], zs_sem)
        arrived(pair, qs_sem)

    anc_copy.wait()
    row0 = pl.multiple_of(lax.rem(z, unit) * rows_z, rows_z)
    for src in range(SOURCES):
        count = pieces * one_each * (split if src else split - 1)
        if src < SOURCES - 1:
            arrived(zsum.at[pl.ds(0, count)], zr_sem.at[src])
        else:
            pl.when(inner)(lambda: arrived(zsum.at[pl.ds(0, count)], zr_sem.at[src]))
            pl.when(jnp.logical_not(inner))(
                lambda: arrived(zsum.at[pl.ds(0, pieces * units * split)], zr_sem.at[src]))
        outermost = far_outer if src < SOURCES - 1 else outer_unit
        for c in range(units):
            flip = outermost == c
            if src == SOURCES - 1:
                flip = jnp.logical_and(flip, inner)

            @pl.when(flip)
            def _():
                turned[...] = t_recv[src].reshape(cols, cols).T
                out[0, :, c * cols:(c + 1) * cols] = (
                    out[0, :, c * cols:(c + 1) * cols] - turned[pl.ds(row0, rows_z)])

            @pl.when(jnp.logical_not(flip))
            def _():
                out[0, :, c * cols:(c + 1) * cols] = (
                    out[0, :, c * cols:(c + 1) * cols] - z_recv[src, c].reshape(rows_z, cols))


def shards(panels, factors, member, target, ancestors):
    sups, blk_count, nb = factors.shape[0], panels.shape[0], member.shape[1]
    width = panels.shape[2]
    n, wide_count = lax.axis_size("narrow"), lax.axis_size("wide")
    side = math.isqrt(wide_count // CORES)
    assert side * side * CORES == wide_count
    tile_count = ancestors.shape[0] * wide_count
    assert ancestors.shape[0] == 1 and n % (CORES * sups) == 0 and nb % 2 == 0 and sups == 2
    assert blk_count == sups * nb
    unit = n // (CORES * sups)
    split = unit * CORES
    part = panels.shape[1] // split
    pieces = max(1, part // PIECE)
    assert pieces <= 2 and n == sups * split
    hr = part // pieces
    units = CORES * sups
    cols = width // units
    f32, bf16 = jnp.float32, jnp.bfloat16
    dma = pltpu.SemaphoreType.DMA
    cfg = (n, side, sups, nb, width, part, unit, split, pieces)
    any_space = pl.BlockSpec(memory_space=pl.ANY)
    smem = pl.BlockSpec(memory_space=pltpu.SMEM)
    return pl.pallas_call(
        functools.partial(kernel, cfg),
        out_shape=jax.ShapeDtypeStruct(ancestors.shape, f32),
        in_specs=[smem, smem, any_space, any_space, any_space],
        out_specs=pl.BlockSpec(memory_space=pltpu.VMEM),
        scratch_shapes=[
            pltpu.VMEM(panels.shape, f32),
            pltpu.VMEM((sups, nb, panels.shape[1], width), f32),
            pltpu.VMEM((n, pieces, nb, hr, width), f32),
            pltpu.VMEM((n, split, part, width), f32),
            pltpu.VMEM((width, width), bf16),
            pltpu.VMEM((width, width), bf16),
            pltpu.VMEM((nb, n, split, part, width), f32),
            pltpu.VMEM((nb, n, split, part, width), bf16),
            pltpu.VMEM((nb, n, split, part, width), bf16),
            pltpu.VMEM((nb * unit * part, nb * cols), f32),
            pltpu.VMEM((units, units, pieces, tile_count, unit, hr, cols), f32),
            pltpu.VMEM((units, units, pieces, side - 1, side * CORES, unit, hr, cols), f32),
            pltpu.VMEM((units, units, pieces, side - 1, CORES, unit, hr, cols), f32),
            pltpu.VMEM((units * units * pieces * CORES * unit * unit, hr, cols), f32),
            pltpu.VMEM((units // 2 * units * pieces * CORES * unit, hr, cols), f32),
            pltpu.VMEM((SOURCES, units, split, pieces, hr, cols), f32),
            pltpu.VMEM((SOURCES, unit, split, pieces, hr, cols), f32),
            pltpu.VMEM((cols, cols), f32),
            pltpu.VMEM((sups * split * pieces, nb, hr, width), f32),
            dma, dma,
            dma, dma,
            dma, dma,
            dma, dma((n, pieces)),
            dma, dma((n, pieces)),
            dma, dma((units, units, side - 1)),
            dma, dma((units, units, side - 1)),
            dma, dma((SOURCES,)),
            dma, dma((pieces + 2,)),
            dma((sups * split * pieces,)), dma,
        ],
        compiler_params=pltpu.CompilerParams(
            collective_id=0, has_side_effects=True, vmem_limit_bytes=58 * 2**20
        ),
        name="level",
    )(member, target, panels, factors, ancestors)


def solution(mesh):
    return jax.shard_map(
        shards,
        mesh=mesh,
        in_specs=(
            P("wide", "narrow", None),
            P("wide", "narrow", None),
            P(),
            P(),
            P("wide", "narrow", None),
        ),
        out_specs=P("wide", "narrow", None),
        check_vma=False,
    )
```

```python
import functools
import math

import jax
import jax.numpy as jnp
from jax import lax
from jax.experimental import pallas as pl
from jax.experimental.pallas import tpu as pltpu
from jax.sharding import PartitionSpec as P

MESH = pl.DeviceIdType.MESH
CORES = 2
PIECE = 32
SOURCES = 3
ROWS_DOT = (((1,), (1,)), ((), ()))
COLS_DOT = (((1,), (0,)), ((), ()))


def halves(x):
    hi = x.astype(jnp.bfloat16)
    return hi, (x - hi.astype(jnp.float32)).astype(jnp.bfloat16)


def dot3(ah, al, bh, bl, dims):
    dot = functools.partial(
        lax.dot_general, dimension_numbers=dims, preferred_element_type=jnp.float32
    )
    return dot(ah, bh) + (dot(ah, bl) + dot(al, bh))


def kernel(cfg, member, target, panels, factors, ancestors, out, pan, stage, p_recv, f_full, fh, fl,
           s_full, s_hi, s_lo, upd, portion, recv1, recv2, zsum, pair, z_recv, t_recv, turned, relay,
           loc_sem, pan_sem, fs_sem, fr_sem, f2s_sem, f2r_sem, ps_sem, pr_sem, ss_sem, sr_sem,
           xs1_sem, xr1_sem, xs2_sem, xr2_sem, zs_sem, zr_sem, qs_sem, qr_sem, rr_sem, rf_sem):
    n, side, sups, nb, width, part, unit, split, pieces = cfg
    hr = part // pieces
    units = CORES * sups
    mid = units // 2
    last = units - 1
    cols = width // units
    rows_z = split * part
    wide = lax.axis_index("wide")
    z = lax.axis_index("narrow")
    core = lax.rem(wide, CORES)
    q = lax.div(wide, CORES)
    mine = lax.rem(z, unit) * CORES + core
    my_unit = lax.div(z, unit)
    half = lax.div(my_unit, mid)
    far_sender = core != half
    outer_unit = half * last
    far_outer = (1 - half) * last
    inner = my_unit != outer_unit
    supernode = q * units + my_unit
    row, col = lax.div(q, side), lax.rem(q, side)

    def at(q_, core_, z_):
        return {"wide": q_ * CORES + core_, "narrow": z_}

    def order(i):
        h, j = i // mid, i % mid
        near = half * mid + lax.rem(my_unit - half * mid + j, mid)
        far = mid + j - half * (1 + 2 * j)
        return (1 - h) * near + h * far

    def remote(src, dst, send, recv, dev):
        return pltpu.make_async_remote_copy(src_ref=src, dst_ref=dst, send_sem=send, recv_sem=recv,
                                            device_id=dev, device_id_type=MESH)

    def arrived(ref, sem):
        pltpu.make_async_copy(ref, ref, sem).wait()

    def piece(h):
        return pl.ds(h * hr if isinstance(h, int) else pl.multiple_of(h * hr, hr), hr)

    pan_copy = pltpu.make_async_copy(panels, pan, pan_sem)
    pan_copy.start()
    anc_copy = pltpu.make_async_copy(ancestors.at[0], out.at[0], loc_sem)
    anc_copy.start()

    barrier = pltpu.get_barrier_semaphore()
    for i in range(1, CORES * n):
        other = lax.rem(z * CORES + core + i, CORES * n)
        pl.semaphore_signal(barrier, inc=1, device_id=at(q, lax.rem(other, CORES), lax.div(other, CORES)),
                            device_id_type=MESH)
    for i in range(1, side):
        for other in (row * side + lax.rem(col + i, side), lax.rem(row + i, side) * side + col):
            pl.semaphore_signal(barrier, inc=1, device_id=at(other, core, z), device_id_type=MESH)
    pl.semaphore_wait(barrier, CORES * n - 1 + 2 * (side - 1))

    def chip_of(s, e):
        return (core * sups + s) * unit + e // CORES

    def to_self(s, e):
        return jnp.logical_and(chip_of(s, e) == z, core == e % CORES)

    def f_source(s, e, local):
        src, dst = factors.at[s, pl.ds(e * part, part)], f_full.at[z, e]
        if local:
            return pltpu.make_async_copy(src, dst, fr_sem)
        return remote(src, dst, fs_sem, fr_sem, at(q, e % CORES, chip_of(s, e)))

    def nearest(i):
        return lax.rem(i + 1 - core, sups)

    def p_source(s, e, h):
        src = stage.at[s, :, pl.ds(e * part + h * hr, hr)]
        return remote(src, p_recv.at[z, h], ps_sem, pr_sem.at[z, h], at(q, e % CORES, chip_of(s, e)))

    parts = [(i, e) for i in range(sups) for e in range(split)]
    for i, e in parts:
        s = nearest(sups - 1 - i)

        @pl.when(to_self(s, e))
        def _():
            f_source(s, e, True).start()

        @pl.when(jnp.logical_not(to_self(s, e)))
        def _():
            f_source(s, e, False).start()

    pan_copy.wait()

    def pick(i, carry):
        s, k = lax.div(i, nb), lax.rem(i, nb)
        stage[s, k] = pan[lax.rem(member[k, wide * sups + s], sups * nb)]
        return carry

    lax.fori_loop(0, sups * nb, pick, 0)

    far_inner = jnp.logical_and(far_sender, inner)
    far_outer_sender = jnp.logical_and(far_sender, jnp.logical_not(inner))
    p_list = [(i, e, h) for i in range(sups) for h in range(pieces) for e in range(split)]
    relay_list = [(i, e, h) for h in range(pieces) for i in reversed(range(sups)) for e in range(split)]
    quarter = len(relay_list) // 4

    def slot(s, e, h):
        return (s * split + e) * pieces + h

    def to_relay(i, e, h):
        s = nearest(i)
        src = stage.at[s, :, pl.ds(e * part + h * hr, hr)]
        return remote(src, relay.at[slot(s, e, h)], ps_sem, rr_sem.at[slot(s, e, h)],
                      at(q, core, z + unit - 2 * unit * half))

    def from_relay(i, e, h):
        s, outer_z = nearest(i), z - unit + 2 * unit * half
        return remote(relay.at[slot(s, e, h)], p_recv.at[outer_z, h], rf_sem, pr_sem.at[outer_z, h],
                      at(q, e % CORES, chip_of(s, e)))

    def send_relay():
        for which in relay_list:
            to_relay(*which).start()

    def pass_on(some):
        for i, e, h in some:
            which = slot(nearest(i), e, h)
            arrived(relay.at[which], rr_sem.at[which])
            from_relay(i, e, h).start()

    def send_panels():
        for i, e, h in p_list:
            s = nearest(i)

            @pl.when(to_self(s, e))
            def _():
                p_recv[z, h] = stage[s, :, pl.ds(e * part + h * hr, hr)]

            @pl.when(jnp.logical_not(to_self(s, e)))
            def _():
                p_source(s, e, h).start()

    pl.when(jnp.logical_not(far_outer_sender))(send_panels)

    arrived(f_full.at[:, mine], fr_sem)

    def peer(i):
        other = lax.rem(mine + i, split)
        return other, at(q, lax.rem(other, CORES), my_unit * unit + lax.div(other, CORES))

    f_copies = []
    for i in range(1, split):
        other, dev = peer(i)
        f_copies.append(remote(f_full.at[:, mine], f_full.at[:, mine], f2s_sem, f2r_sem, dev))
        f_copies[-1].start()
    others = pl.ds(0, split - 1)
    arrived(f_full.at[:, others], f2r_sem)
    hi, lo = halves(f_full[...].reshape(width, width))
    fh[...] = hi
    fl[...] = lo

    def s_copy(zz, h, j):
        other, dev = peer(j)
        ref = s_full.at[:, zz, mine, piece(h)]
        return remote(ref, ref, ss_sem, sr_sem.at[zz, h], dev)

    def scale(zz, h):
        @pl.when(jnp.logical_not(jnp.logical_and(zz == z, core == half)))
        def _():
            arrived(p_recv.at[zz, h], pr_sem.at[zz, h])

        ph, plo = halves(p_recv[zz, h].reshape(nb * hr, width))
        s = dot3(ph, plo, fh[...], fl[...], COLS_DOT).reshape(nb, hr, width)
        s_full[:, zz, mine, piece(h)] = s
        for j in range(1, split):
            s_copy(zz, h, j).start()
        s_hi[:, zz, mine, piece(h)], s_lo[:, zz, mine, piece(h)] = halves(s)

    def take(zz, h):
        arrived(s_full.at[:, zz, others, piece(h)], sr_sem.at[zz, h])
        for j in range(1, split):
            other, _ = peer(j)
            s_hi[:, zz, other, piece(h)], s_lo[:, zz, other, piece(h)] = halves(s_full[:, zz, other, piece(h)])

    def scale_all(a, between=None):
        def one(i, carry):
            scale(a * unit + lax.div(i, pieces), lax.rem(i, pieces))
            return carry

        def two(i, carry):
            take(a * unit + lax.div(i, pieces), lax.rem(i, pieces))
            return carry

        lax.fori_loop(0, unit * pieces, one, 0)
        if between is not None:
            between()
        lax.fori_loop(0, unit * pieces, two, 0)

    def place(r, c, h):
        along_row = jnp.logical_or(r > c, jnp.logical_and(r == c, h == 0))
        return along_row, jnp.where(along_row, col, row), jnp.where(along_row, row, col)

    def q_at(along_row, f, g):
        return jnp.where(along_row, g * side + f, f * side + g)

    def steps(src, dst):
        return lax.rem(src - dst - 1 + side, side)

    def mark(r, c, h):
        in_pieces = jnp.logical_and(r != c, jnp.logical_or(r == far_outer, c == far_outer))
        other = r + c - far_outer
        return (jnp.where(in_pieces, jnp.where(h == 0, far_outer, other), r),
                jnp.where(in_pieces, jnp.where(h == 0, other, far_outer), c))

    def first_copy(r, c, h, f):
        along_row, mine_f, mine_g = place(r, c, h)
        d = steps(mine_f, f)
        return remote(portion.at[r, c, h, pl.ds(f * side * CORES, side * CORES)], recv1.at[r, c, h, d],
                      xs1_sem, xr1_sem.at[*mark(r, c, h), d], at(q_at(along_row, f, mine_g), core, z))

    def second_copy(r, c, h, g):
        along_row, mine_f, mine_g = place(r, c, h)
        d = steps(mine_g, g)
        return remote(portion.at[r, c, h, pl.ds((mine_f * side + g) * CORES, CORES)], recv2.at[r, c, h, d],
                      xs2_sem, xr2_sem.at[*mark(r, c, h), d], at(q_at(along_row, mine_f, g), core, z))

    two = nb // 2

    def products(a, b, h=None):
        rows = unit * (part if h is None else hr)
        bz, az = pl.ds(b * unit, unit), pl.ds(a * unit, unit)
        for first in range(0, nb, two):
            low = first if h is None else 0
            ks, ls = pl.ds(low, nb - low), pl.ds(first, two)
            left = [(r[ks, az, mine] if h is None else r[ks, az, mine, piece(h)]).reshape((nb - low) * rows, width)
                    for r in (s_hi, s_lo)]
            right = [r[ls, bz].reshape(two * cols, width) for r in (s_hi, s_lo)]
            upd[low * rows:nb * rows, first * cols:(first + two) * cols] = dot3(*left, *right, ROWS_DOT)

    def sums_of(r, c, h=None, flip=False):
        hs = range(pieces) if h is None else (h,)
        rows = unit * len(hs) * hr

        def tiles(i, carry):
            i = lax.rem(q + 1 + i, side * side)
            oq, og = lax.div(i, side), lax.rem(i, side)
            sums = [None] * CORES
            p = 0
            for k in range(nb):
                for l in range(k + 1):
                    x, y = (l, k) if flip else (k, l)
                    u = upd[x * rows:(x + 1) * rows, y * cols:(y + 1) * cols]
                    for t in range(CORES):
                        term = (target[supernode, p] == i * CORES + t).astype(jnp.float32) * u
                        sums[t] = term if p == 0 else sums[t] + term
                    p += 1
            for x, hh in enumerate(hs):
                along_row, mine_f, mine_g = place(r, c, hh)
                f, g = jnp.where(along_row, og, oq), jnp.where(along_row, oq, og)
                for t in range(CORES):
                    for m in range(unit):
                        first = (m * len(hs) + x) * hr
                        portion[r, c, hh, (f * side + g) * CORES + t, m] = sums[t][first:first + hr]
            return carry

        lax.fori_loop(0, side * side, tiles, 0)
        for hh in hs:
            _, mine_f, _ = place(r, c, hh)
            for j in range(1, side):
                first_copy(r, c, hh, lax.rem(mine_f + j, side)).start()

    def block(a, b):
        products(a, b)
        sums_of(a, b)

    def item(i, j):
        new_row = j <= i
        return (order(jnp.where(new_row, i, j - i - 1)), order(jnp.where(new_row, j, i)))

    def step(i):
        scale_all(order(i), (lambda: pl.when(far_outer_sender)(send_relay)) if i == 1 else None)

        def one(j, carry):
            block(*item(i, j))
            return carry

        lax.fori_loop(0, 2 * i + 1, one, 0)

    def last_step(h, between=None):
        for m in range(unit):
            scale(far_outer * unit + m, h)
        if between is not None:
            between()
        for m in range(unit):
            take(far_outer * unit + m, h)

        def one(j, carry):
            products(far_outer, order(j), h)
            sums_of(far_outer, order(j), h)
            sums_of(order(j), far_outer, h, True)
            return carry

        lax.fori_loop(0, last, one, 0)

    def is_near(r):
        return lax.div(r, mid) == half

    def total_at(r, c, h, t=0, m=0):
        return (((r * units + c) * pieces + h) * CORES + t) * unit + m

    def deliver(r, c, h):
        near = is_near(r)
        src = jnp.where(near, jnp.where(r == my_unit, 0, 1), SOURCES - 1)
        flip = jnp.logical_and(c == far_outer, r != far_outer)
        for t in range(CORES):
            for m in range(unit):
                zz = r * unit + m
                own = jnp.logical_and(zz == z, core == t)
                send, recv, dev = zs_sem, zr_sem.at[src], at(q, t, zz)
                plain = remote(zsum.at[total_at(r, c, h, t, m)], z_recv.at[src, c, mine, h], send, recv, dev)
                flipped = remote(zsum.at[pl.ds(total_at(r, c, h, t), unit)], t_recv.at[src, :, mine, h], send, recv, dev)

                @pl.when(jnp.logical_and(own, jnp.logical_not(flip)))
                def _():
                    z_recv[0, c, mine, h] = zsum[total_at(r, c, h, t, m)]

                @pl.when(jnp.logical_and(own, flip))
                def _():
                    t_recv[0, :, mine, h] = zsum[pl.ds(total_at(r, c, h, t), unit)]

                @pl.when(jnp.logical_and(jnp.logical_not(own), jnp.logical_not(flip)))
                def _():
                    plain.start()

                @pl.when(jnp.logical_and(jnp.logical_not(own), flip))
                def _():
                    flipped.start()

    both = CORES * unit

    def sums_at(r, c, h):
        return pl.ds(total_at(r, c, h), both)

    def pair_copy(r, c, h, phase):
        return remote(zsum.at[sums_at(r, c, h)], pair.at[sums_at(lax.rem(r, mid), c, h)], qs_sem, qr_sem.at[phase],
                      at(q, core, z + unit - 2 * unit * half))

    def halfway(r, c, h):
        _, mine_f, mine_g = place(r, c, h)
        own = pl.ds(mine_f * side * CORES, side * CORES)
        total = portion[r, c, h, own]
        for d in range(side - 1):
            total = total + recv1[r, c, h, d]
        portion[r, c, h, own] = total
        for j in range(1, side):
            second_copy(r, c, h, lax.rem(mine_g + j, side)).start()

    def gather(r, c, h, phase):
        _, mine_f, mine_g = place(r, c, h)
        total = portion[r, c, h, pl.ds((mine_f * side + mine_g) * CORES, CORES)]
        for d in range(side - 1):
            total = total + recv2[r, c, h, d]
        zsum[sums_at(r, c, h)] = total.reshape(both, hr, cols)

        @pl.when(is_near(r))
        def _():
            deliver(r, c, h)

        @pl.when(jnp.logical_not(jnp.logical_or(is_near(r), inner)))
        def _():
            pair_copy(r, c, h, phase).start()

    def join(r, c, h):
        @pl.when(jnp.logical_not(is_near(r)))
        def _():
            zsum[sums_at(r, c, h)] = zsum[sums_at(r, c, h)] + pair[sums_at(lax.rem(r, mid), c, h)]
            deliver(r, c, h)

    def came(recv, sem, r, c, h=None):
        for d in range(side - 1):
            ref = recv.at[r, c, :, d] if h is None else recv.at[0, pl.ds(0, 2), 0, d]
            arrived(ref, sem.at[*(mark(r, c, h) if h is not None else (r, c)), d])

    def over(do, i, recv=None, sem=None):
        def one(j, carry):
            r, c = item(i, j)
            if sem is not None:
                came(recv, sem, r, c)
            for h in range(pieces):
                do(r, c, h)
            return carry

        lax.fori_loop(0, 2 * i + 1, one, 0)

    def over_last(do, h, recv=None, sem=None):
        def one(j, carry):
            a = order(j)
            if sem is not None:
                came(recv, sem, far_outer, a, h)
            do(far_outer, a, h)
            do(a, far_outer, h)
            return carry

        lax.fori_loop(0, last, one, 0)

    def over_corner(do, recv=None, sem=None):
        if sem is not None:
            came(recv, sem, far_outer, far_outer)
        for h in range(pieces):
            do(far_outer, far_outer, h)

    def in_phase(phase):
        return lambda r, c, h: gather(r, c, h, phase)

    def joined(phase, count, run):
        @pl.when(inner)
        def _():
            arrived(pair.at[pl.ds(0, count * both)], qr_sem.at[phase])
            run()

    step(0)
    step(1)
    pl.when(far_inner)(lambda: pass_on(relay_list[:2 * quarter]))
    over(halfway, 0, recv1, xr1_sem)
    over(halfway, 1, recv1, xr1_sem)
    step(2)
    pl.when(far_inner)(lambda: pass_on(relay_list[2 * quarter:3 * quarter]))
    over(in_phase(0), 0, recv2, xr2_sem)
    over(in_phase(0), 1, recv2, xr2_sem)
    for h in range(pieces - 1):
        last_step(h)
        if h == 0:
            pl.when(far_inner)(lambda: pass_on(relay_list[3 * quarter:]))
        over(halfway, 2, recv1, xr1_sem)
        over_last(halfway, h, recv1, xr1_sem)
    if pieces == 1:
        pl.when(far_inner)(lambda: pass_on(relay_list[3 * quarter:]))
        over(halfway, 2, recv1, xr1_sem)
    last_step(pieces - 1, lambda: over(in_phase(0), 2, recv2, xr2_sem))
    joined(0, last * pieces, lambda: over(join, 2))
    block(far_outer, far_outer)
    for h in range(pieces - 1):
        over_last(in_phase(1 + h), h, recv2, xr2_sem)
    over_last(halfway, pieces - 1, recv1, xr1_sem)
    for h in range(pieces - 1):
        joined(1 + h, last + 1, lambda h=h: over_last(join, h))
    over_corner(halfway, recv1, xr1_sem)
    over_last(in_phase(pieces), pieces - 1, recv2, xr2_sem)
    joined(pieces, last + 1, lambda: over_last(join, pieces - 1))
    over_corner(in_phase(pieces + 1), recv2, xr2_sem)
    joined(pieces + 1, pieces, lambda: over_corner(join))

    one_each = last + unit
    pl.when(far_sender)(lambda: arrived(f_full.at[:, 0], fs_sem))
    pl.when(jnp.logical_not(far_sender))(lambda: arrived(f_full.at[pl.ds(0, n - 1), 0], fs_sem))
    pl.when(far_sender)(lambda: arrived(relay, ps_sem))
    pl.when(jnp.logical_not(far_sender))(lambda: arrived(relay.at[pl.ds(0, (n - 1) * pieces)], ps_sem))
    pl.when(far_inner)(lambda: arrived(relay, rf_sem))
    arrived(f_full.at[:, others], f2s_sem)
    arrived(s_full.at[:, :, others], ss_sem)
    arrived(recv1, xs1_sem)
    arrived(recv2, xs2_sem)
    near_count = pieces * one_each * (mid * both - 1)
    far_count = pieces * both * (one_each + (mid - 1) * units)
    pl.when(inner)(lambda: arrived(zsum.at[pl.ds(0, near_count + far_count)], zs_sem))

    @pl.when(jnp.logical_not(inner))
    def _():
        arrived(zsum.at[pl.ds(0, near_count)], zs_sem)
        arrived(pair, qs_sem)

    anc_copy.wait()
    row0 = pl.multiple_of(lax.rem(z, unit) * rows_z, rows_z)
    for src in range(SOURCES):
        count = pieces * one_each * (split if src else split - 1)
        if src < SOURCES - 1:
            arrived(zsum.at[pl.ds(0, count)], zr_sem.at[src])
        else:
            pl.when(inner)(lambda: arrived(zsum.at[pl.ds(0, count)], zr_sem.at[src]))
            pl.when(jnp.logical_not(inner))(
                lambda: arrived(zsum.at[pl.ds(0, pieces * units * split)], zr_sem.at[src]))
        outermost = far_outer if src < SOURCES - 1 else outer_unit
        for c in range(units):
            flip = outermost == c
            if src == SOURCES - 1:
                flip = jnp.logical_and(flip, inner)

            @pl.when(flip)
            def _():
                turned[...] = t_recv[src].reshape(cols, cols).T
                out[0, :, c * cols:(c + 1) * cols] = (
                    out[0, :, c * cols:(c + 1) * cols] - turned[pl.ds(row0, rows_z)])

            @pl.when(jnp.logical_not(flip))
            def _():
                out[0, :, c * cols:(c + 1) * cols] = (
                    out[0, :, c * cols:(c + 1) * cols] - z_recv[src, c].reshape(rows_z, cols))


def shards(panels, factors, member, target, ancestors):
    sups, blk_count, nb = factors.shape[0], panels.shape[0], member.shape[1]
    width = panels.shape[2]
    n, wide_count = lax.axis_size("narrow"), lax.axis_size("wide")
    side = math.isqrt(wide_count // CORES)
    assert side * side * CORES == wide_count
    tile_count = ancestors.shape[0] * wide_count
    assert ancestors.shape[0] == 1 and n % (CORES * sups) == 0 and nb % 2 == 0 and sups == 2
    assert blk_count == sups * nb
    unit = n // (CORES * sups)
    split = unit * CORES
    part = panels.shape[1] // split
    pieces = max(1, part // PIECE)
    assert pieces <= 2 and n == sups * split
    hr = part // pieces
    units = CORES * sups
    cols = width // units
    f32, bf16 = jnp.float32, jnp.bfloat16
    dma = pltpu.SemaphoreType.DMA
    cfg = (n, side, sups, nb, width, part, unit, split, pieces)
    any_space = pl.BlockSpec(memory_space=pl.ANY)
    smem = pl.BlockSpec(memory_space=pltpu.SMEM)
    return pl.pallas_call(
        functools.partial(kernel, cfg),
        out_shape=jax.ShapeDtypeStruct(ancestors.shape, f32),
        in_specs=[smem, smem, any_space, any_space, any_space],
        out_specs=pl.BlockSpec(memory_space=pltpu.VMEM),
        scratch_shapes=[
            pltpu.VMEM(panels.shape, f32),
            pltpu.VMEM((sups, nb, panels.shape[1], width), f32),
            pltpu.VMEM((n, pieces, nb, hr, width), f32),
            pltpu.VMEM((n, split, part, width), f32),
            pltpu.VMEM((width, width), bf16),
            pltpu.VMEM((width, width), bf16),
            pltpu.VMEM((nb, n, split, part, width), f32),
            pltpu.VMEM((nb, n, split, part, width), bf16),
            pltpu.VMEM((nb, n, split, part, width), bf16),
            pltpu.VMEM((nb * unit * part, nb * cols), f32),
            pltpu.VMEM((units, units, pieces, tile_count, unit, hr, cols), f32),
            pltpu.VMEM((units, units, pieces, side - 1, side * CORES, unit, hr, cols), f32),
            pltpu.VMEM((units, units, pieces, side - 1, CORES, unit, hr, cols), f32),
            pltpu.VMEM((units * units * pieces * CORES * unit * unit, hr, cols), f32),
            pltpu.VMEM((units // 2 * units * pieces * CORES * unit, hr, cols), f32),
            pltpu.VMEM((SOURCES, units, split, pieces, hr, cols), f32),
            pltpu.VMEM((SOURCES, unit, split, pieces, hr, cols), f32),
            pltpu.VMEM((cols, cols), f32),
            pltpu.VMEM((sups * split * pieces, nb, hr, width), f32),
            dma, dma,
            dma, dma,
            dma, dma,
            dma, dma((n, pieces)),
            dma, dma((n, pieces)),
            dma, dma((units, units, side - 1)),
            dma, dma((units, units, side - 1)),
            dma, dma((SOURCES,)),
            dma, dma((pieces + 2,)),
            dma((sups * split * pieces,)), dma,
        ],
        compiler_params=pltpu.CompilerParams(
            collective_id=0, has_side_effects=True, vmem_limit_bytes=54912 * 2**10
        ),
        name="level",
    )(member.T, target, panels, factors, ancestors)


def solution(mesh):
    return jax.shard_map(
        shards,
        mesh=mesh,
        in_specs=(
            P("wide", "narrow", None),
            P("wide", "narrow", None),
            P(),
            P(),
            P("wide", "narrow", None),
        ),
        out_specs=P("wide", "narrow", None),
        check_vma=False,
    )
```
